256 devices in a mesh: cuts: 4 (over y, x), wide: 32 (over z), batch: 2 (over core).
Axes of the slice: x: 2, y: 2, z: 32, core: 2. Of those that a mesh axis runs over, the one named last changes fastest.
The devices are a block of a 4x8x32 slice.
Arguments:
- initial: bfloat16 [2, 128, 2, 2, 256, 256], P('batch', 'cuts', None, None, None, 'wide'), parts along dimension 1, may hold values from -6 to 6
- branches: bfloat16 [8, 2, 2, 256, 2, 256], P(None, None, None, 'batch'), may hold values from -0.1875 to 0.1875
- projectors: float32 [8, 2, 2, 2], replicated, may hold values from -4 to 4
- bits: int32 [2, 8], P('batch'), may hold values from 0 to 1
Outputs:
- amplitudes: float32 [2, 128, 2, 2, 256, 256], P('batch', 'cuts', None, None, 'wide'), parts along dimension 1
The draws below stay inside these ranges and needn't reach their ends.
There are 4 independent parts, one for each index of `cuts`. The reference program is written for one: setup_inputs(seed, part) draws one part's arguments, and reference() takes and returns one part's arrays. A program takes and returns all parts, laid end to end along the dimension named above; an argument that names none is the same for every part. Nothing has to cross between parts.
Inputs may be any that keep to these rules, and one draw needn't show every extreme that they name: `bits`: each entry is a bit.
All inputs are finite; a program needn't handle non-finite values.
Results may differ from the reference program's by a relative error of at most 0.014.
Values may be sent and summed in bfloat16 or wider, within the bound.
A program may use at most 64 MiB of HBM per device.

```python
import jax
import jax.numpy as jnp

QGROUP = 256
HSHARED = 2
COLUMNS = 32
STEPS = 8
BATCH = 2


def set_ends(values, own_key, least, largest):
    dims = values.shape
    place = [jax.random.randint(jax.random.fold_in(own_key, axis), (), 0, dims[axis]) for axis in range(len(dims))]
    values = values.at[tuple(place)].set(least)
    longest = dims.index(max(dims))
    place[longest] = (place[longest] + 1) % dims[longest]
    return values.at[tuple(place)].set(largest)


def level_of(rng, extent, split, smallest, top_value):
    factor_of, own = 1.0, jax.random.fold_in(rng, 6)
    for dim, shards_of in split:
        steps = jnp.exp(jax.random.uniform(jax.random.fold_in(own, dim), (shards_of,), jnp.float32, smallest / len(split), top_value / len(split)))
        factor_of = factor_of * jnp.repeat(steps, extent[dim] // shards_of).reshape([-1 if axis == dim else 1 for axis in range(len(extent))])
    return factor_of


def scatter_about(rng, dims, deviation, limit, pieces=(), kind=jnp.bfloat16):
    values = jax.random.normal(rng, dims, jnp.float32) * deviation
    if len(pieces) > 0:
        values = level_of(rng, dims, pieces, -0.22, 0.18) * values
    return jnp.clip(values, min=-limit, max=limit).astype(kind)


def setup_inputs(seed: int = 0, part: int = 0) -> dict:
    keys = jax.random.split(jax.random.key(seed), 5)
    part_keys = jax.random.split(jax.random.fold_in(keys[4], part), 5)
    initial = scatter_about(part_keys[0], (BATCH, COLUMNS, 2, HSHARED, QGROUP, QGROUP), 1.0, 6.0, ((0, 2), (5, 32)))
    branches = scatter_about(keys[1], (STEPS, 2, HSHARED, QGROUP, HSHARED, QGROUP), (2 * HSHARED * QGROUP) ** -0.5, 0.1875, ((3, 2),))
    projectors = scatter_about(keys[2], (STEPS, 2, 2, HSHARED), 0.7, 4.0, (), jnp.float32)
    bits = set_ends(jax.random.randint(keys[3], (BATCH, STEPS), 0, 2), jax.random.fold_in(keys[3], 1), 0, 1).astype(jnp.int32)
    return {"initial": initial, "branches": branches, "projectors": projectors, "bits": bits}


def contract(state, branch, select):
    prod = jnp.einsum('ncphuv,thugw->ncptgvw', state.astype(jnp.float32), branch.astype(jnp.float32))
    real_part = prod[:, :, 0, 0] - prod[:, :, 1, 1]
    imag_part = prod[:, :, 0, 1] + prod[:, :, 1, 0]
    proj_re = select[:, 0][:, None, :, None, None]
    proj_im = select[:, 1][:, None, :, None, None]
    out_re = proj_re * real_part - proj_im * imag_part
    out_im = proj_re * imag_part + proj_im * real_part
    return jnp.stack([out_re, out_im], axis=2)


def reference(initial, branches, projectors, bits):
    state = initial
    result = None
    for step in range(STEPS):
        chosen = (bits[:, step] == 1)[:, None, None]
        select = jnp.where(chosen, projectors[step, 1][None], projectors[step, 0][None])
        result = contract(state, branches[step], select)
        state = result.astype(jnp.bfloat16)
    return result
```

```python
import functools

import jax
import jax.numpy as jnp
from jax import lax
from jax.experimental import pallas as pl
from jax.experimental.pallas import tpu as pltpu
from jax.sharding import PartitionSpec as P

MESH = pl.DeviceIdType.MESH
BF16, F32 = jnp.bfloat16, jnp.float32


def dot(a, b, dims=((1,), (0,))):
    return lax.dot_general(a, b, (dims, ((), ())), preferred_element_type=F32)


def hops_of(n):
    order = [(n // 2, 0), (-(n // 2), 1)]
    for far in range(n // 2 - 1, 0, -1):
        order += [(far, None), (-far, None)]
    return order


def kernel(n, x_hbm, b_hbm, p_hbm, bits_hbm, out, parts, even_w, odd_w, rows_t, rows, send, last, p_s, bits_s,
           send1, recv1, send2, recv2, bsend, brecv, bown, small):
    z = lax.axis_index("wide")
    core = lax.axis_index("batch")
    wide, cols = x_hbm.shape[0] // n, x_hbm.shape[1]
    group = cols // 4
    steps = b_hbm.shape[0]
    hops = hops_of(n)

    barrier = pltpu.get_barrier_semaphore()
    pl.semaphore_signal(barrier, inc=1, device_id={"batch": 1 - core}, device_id_type=MESH)
    for d in range(1, n):
        pl.semaphore_signal(barrier, inc=1, device_id={"wide": lax.rem(z + d, n)}, device_id_type=MESH)
    pl.semaphore_wait(barrier, n)

    def block(ref, index, piece):
        at = pl.ds(pl.multiple_of(index * wide, wide), wide)
        if piece is None:
            return ref.at[at, :]
        return ref.at[at, pl.ds(piece * (cols // 2), cols // 2)]

    def exchange(src, dst, ssem, rsem):
        copies = []
        for i, (d, piece) in enumerate(hops):
            to = lax.rem(z + d + n, n)
            copies.append(pltpu.make_async_remote_copy(
                src_ref=block(src, to, piece), dst_ref=block(dst, z, piece), send_sem=ssem.at[i], recv_sem=rsem.at[i],
                device_id={"wide": to}, device_id_type=MESH))
        return copies

    first = exchange(x_hbm, rows_t, send1, recv1)
    for copy in first:
        copy.start()

    def push(s):
        return pltpu.make_async_remote_copy(
            src_ref=b_hbm.at[s], dst_ref=parts.at[core, s], send_sem=bsend.at[s], recv_sem=brecv.at[s],
            device_id={"batch": 1 - core}, device_id_type=MESH)

    def pull(s):
        return pltpu.make_async_copy(b_hbm.at[s], parts.at[core, s], bown.at[s])

    for s in range(steps):
        push(s).start()
        pull(s).start()
    local = [pltpu.make_async_copy(p_hbm, p_s, small.at[0]), pltpu.make_async_copy(bits_hbm, bits_s, small.at[1]),
             pltpu.make_async_copy(block(x_hbm, z, None), block(rows_t, z, None), small.at[2])]
    for copy in local:
        copy.start()

    depth, lanes = b_hbm.shape[3], b_hbm.shape[4]
    half = group // 2
    quarter = half // 2

    def arrived(s):
        pull(s).wait()
        push(s).wait_recv()

    def pair(h, s, uh, at):
        return jnp.concatenate([parts[uh, s, 0, h, at, :], parts[uh, s, 1, h, at, :]], axis=1)

    def one_hot(shape, hit):
        return jnp.where(hit(lax.broadcasted_iota(jnp.int32, shape, 0), lax.broadcasted_iota(jnp.int32, shape, 1)), 1.0, 0.0).astype(BF16)

    def prepare_even(i, s):
        perm = one_hot((2 * half, 2 * half), lambda j, r: r == (j % quarter) * 4 + j // quarter)
        for h in range(2):
            for uh in range(2):
                for ub in range(2):
                    got = dot(perm, pair(h, s, uh, pl.ds(ub * 4 * quarter, 4 * quarter))).astype(BF16)
                    for wt in range(2):
                        for g in range(2):
                            k = (wt * 2 + g) * quarter
                            re, im = got[k:k + quarter, :lanes], got[k:k + quarter, lanes:]
                            u = uh * half + ub * quarter
                            for p, q, what in ((0, 0, re), (0, 1, im), (1, 0, -im), (1, 1, re)):
                                even_w[i, pl.ds((p * 2 + h) * group + u, quarter), pl.ds((q * 2 + g) * group + wt * lanes, lanes)] = what

    def prepare_odd(i, s):
        perm = one_hot((depth, depth), lambda r, j: r == (j % half) * 4 + j // half)
        for h in range(2):
            for uh in range(2):
                got = dot(pair(h, s, uh, slice(None)), perm, ((0,), (0,))).astype(BF16)
                for wt in range(2):
                    for g in range(2):
                        k = (wt * 2 + g) * half
                        re, im = got[:lanes, k:k + half], got[lanes:, k:k + half]
                        for p, q, what in ((0, 0, re), (0, 1, im), (1, 0, -im), (1, 1, re)):
                            odd_w[i, pl.ds((q * 2 + g) * group + wt * lanes, lanes), pl.ds((p * 2 + h) * group + uh * half, half)] = what

    def prepare(i, _):
        arrived(2 * i)
        prepare_even(i, 2 * i)
        arrived(2 * i + 1)
        prepare_odd(i, 2 * i + 1)
        return 0

    lax.fori_loop(0, 3, prepare, 0)
    arrived(6)
    prepare_odd(3, 6)

    for copy in local:
        copy.wait()

    def project(s, g, y_re, y_im):
        one = bits_s[0, s] == 1
        p_re = jnp.where(one, p_s[1, 0, g, s], p_s[0, 0, g, s])
        p_im = jnp.where(one, p_s[1, 1, g, s], p_s[0, 1, g, s])
        return p_re * y_re - p_im * y_im, p_re * y_im + p_im * y_re

    def at(q, g):
        return pl.ds((q * 2 + g) * group, group)

    for copy in first:
        copy.wait_recv()

    def two_steps(i, _):
        for g in range(2):
            z_re, z_im = project(2 * i, g, dot(rows_t[...], even_w[i, :, at(0, g)]), dot(rows_t[...], even_w[i, :, at(1, g)]))
            rows[at(0, g), :] = z_re.astype(BF16)
            rows[at(1, g), :] = z_im.astype(BF16)
        for g in range(2):
            z_re, z_im = project(2 * i + 1, g, dot(odd_w[i, at(0, g), :], rows[...]), dot(odd_w[i, at(1, g), :], rows[...]))
            rows_t[:, at(0, g)] = z_re.astype(BF16)
            rows_t[:, at(1, g)] = z_im.astype(BF16)
        return 0

    lax.fori_loop(0, 3, two_steps, 0)
    for g in range(2):
        z_re, z_im = project(6, g, dot(odd_w[3, at(0, g), :], rows_t[...], ((1,), (1,))),
                             dot(odd_w[3, at(1, g), :], rows_t[...], ((1,), (1,))))
        send[:, at(0, g)] = z_re.astype(BF16)
        send[:, at(1, g)] = z_im.astype(BF16)

    second = exchange(send, last, send2, recv2)
    for copy in second:
        copy.start()
    own = pltpu.make_async_copy(block(send, z, None), block(last, z, None), small.at[0])
    own.start()
    arrived(7)
    prepare_even(3, 7)
    for s in range(steps):
        push(s).wait_send()
    for copy in first:
        copy.wait_send()
    own.wait()
    for copy in second:
        copy.wait_recv()
    for g in range(2):
        z_re, z_im = project(7, g, dot(last[...], even_w[3, :, at(0, g)]), dot(last[...], even_w[3, :, at(1, g)]))
        out[0, :, 0, g] = z_re.reshape(n, wide, group)
        out[0, :, 1, g] = z_im.reshape(n, wide, group)
    for copy in second:
        copy.wait_send()


def shards(n, initial, branches, projectors, bits):
    _, columns, _, _, group, wide = initial.shape
    steps, _, _, half, _, _ = branches.shape
    x = initial[0].transpose(0, 4, 1, 2, 3).reshape(columns * wide, 4 * group)
    b = branches.reshape(steps, 2, 2, half, 2, 2, group // 2).transpose(0, 1, 2, 3, 5, 4, 6).reshape(steps, 2, 2, half * 4, group // 2)
    hops = len(hops_of(n))
    return pl.pallas_call(
        functools.partial(kernel, n),
        out_shape=jax.ShapeDtypeStruct((1, columns, 2, 2, wide, group), F32),
        in_specs=[pl.BlockSpec(memory_space=pl.ANY)] * 4,
        out_specs=pl.BlockSpec(memory_space=pltpu.VMEM),
        scratch_shapes=[
            pltpu.VMEM((2, steps, 2, 2, half * 4, group // 2), BF16),
            pltpu.VMEM((4, 4 * group, 4 * group), BF16),
            pltpu.VMEM((4, 4 * group, 4 * group), BF16),
            pltpu.VMEM((group, 4 * group), BF16),
            pltpu.VMEM((4 * group, group), BF16),
            pltpu.VMEM((group, 4 * group), BF16),
            pltpu.VMEM((group, 4 * group), BF16),
            pltpu.SMEM((2, 2, 2, steps), F32),
            pltpu.SMEM((1, steps), jnp.int32),
            pltpu.SemaphoreType.DMA((hops,)),
            pltpu.SemaphoreType.DMA((hops,)),
            pltpu.SemaphoreType.DMA((hops,)),
            pltpu.SemaphoreType.DMA((hops,)),
            pltpu.SemaphoreType.DMA((steps,)),
            pltpu.SemaphoreType.DMA((steps,)),
            pltpu.SemaphoreType.DMA((steps,)),
            pltpu.SemaphoreType.DMA((3,)),
        ],
        compiler_params=pltpu.CompilerParams(collective_id=0, has_side_effects=True, vmem_limit_bytes=60 * 2**20),
    )(x, b, projectors.transpose(1, 2, 3, 0), bits)


def solution(mesh):
    in_specs = (
        P("batch", "cuts", None, None, None, "wide"),
        P(None, None, None, "batch", None, None),
        P(),
        P("batch", None),
    )
    out_specs = P("batch", "cuts", None, None, "wide", None)
    return jax.shard_map(functools.partial(shards, mesh.shape["wide"]), mesh=mesh, in_specs=in_specs, out_specs=out_specs, check_vma=False)
```

```python
import functools

import jax
import jax.numpy as jnp
from jax import lax
from jax.experimental import pallas as pl
from jax.experimental.pallas import tpu as pltpu
from jax.sharding import PartitionSpec as P

MESH = pl.DeviceIdType.MESH
BF16, F32 = jnp.bfloat16, jnp.float32


def dot(a, b, dims=((1,), (0,))):
    return lax.dot_general(a, b, (dims, ((), ())), preferred_element_type=F32)


def hops_of(n):
    order = [(n // 2, 0), (-(n // 2), 1)]
    for far in range(n // 2 - 1, 0, -1):
        order += [(far, None), (-far, None)]
    return order


NEAR = 3


def chain_of(n):
    reach, rounds = min(NEAR, n // 2), []
    while reach < n // 2:
        rounds.append(min(reach, n // 2 - reach))
        reach += rounds[-1]
    return rounds


def kernel(n, x_hbm, b_hbm, p_hbm, bits_hbm, out, parts, even_w, odd_w, rows_t, rows, send, last, p_s, bits_s,
           send1, recv1, send2, recv2, bsend, brecv, bown, small, chain):
    z = lax.axis_index("wide")
    core = lax.axis_index("batch")
    wide, cols = x_hbm.shape[0] // n, x_hbm.shape[1]
    group = cols // 4
    steps = b_hbm.shape[0]
    hops = hops_of(n)

    barrier = pltpu.get_barrier_semaphore()
    pl.semaphore_signal(barrier, inc=1, device_id={"batch": 1 - core}, device_id_type=MESH)
    for d in range(1, NEAR + 1):
        for to in (d, n - d):
            pl.semaphore_signal(barrier, inc=1, device_id={"wide": lax.rem(z + to, n)}, device_id_type=MESH)
    pl.semaphore_wait(barrier, 2 * NEAR + 1)

    def block(ref, index, piece):
        at = pl.ds(pl.multiple_of(index * wide, wide), wide)
        if piece is None:
            return ref.at[at, :]
        return ref.at[at, pl.ds(piece * (cols // 2), cols // 2)]

    def exchange(src, dst, ssem, rsem):
        copies = []
        for i, (d, piece) in enumerate(hops):
            to = lax.rem(z + d + n, n)
            copies.append(pltpu.make_async_remote_copy(
                src_ref=block(src, to, piece), dst_ref=block(dst, z, piece), send_sem=ssem.at[i], recv_sem=rsem.at[i],
                device_id={"wide": to}, device_id_type=MESH))
        return copies

    def push(s):
        return pltpu.make_async_remote_copy(
            src_ref=b_hbm.at[s], dst_ref=parts.at[core, s], send_sem=bsend.at[s], recv_sem=brecv.at[s],
            device_id={"batch": 1 - core}, device_id_type=MESH)

    def pull(s):
        return pltpu.make_async_copy(b_hbm.at[s], parts.at[core, s], bown.at[s])

    first = exchange(x_hbm, rows_t, send1, recv1)

    def start(nearest, farthest):
        for (d, _), copy in reversed(list(zip(hops, first))):
            if nearest <= abs(d) <= farthest:
                copy.start()

    rounds = chain_of(n)
    reach = NEAR
    start(1, reach)
    for s in range(steps):
        push(s).start()
        pull(s).start()
    near = 2 * NEAR
    for k, hop in enumerate(rounds):
        pl.semaphore_signal(chain.at[k, 0], inc=1, device_id={"wide": lax.rem(z + hop, n)}, device_id_type=MESH)
        pl.semaphore_signal(chain.at[k, 1], inc=1, device_id={"wide": lax.rem(z + n - hop, n)}, device_id_type=MESH)
        pl.semaphore_wait(chain.at[k, 0], 1)
        pl.semaphore_wait(chain.at[k, 1], 1)
        if reach < near:
            start(reach + 1, near)
        reach += hop

    def rest(odd):
        for dests in (0, 1):
            for (d, _), copy in zip(hops, first):
                if abs(d) > near and (d + odd + dests) % 2 == 0:
                    copy.start()

    @pl.when(lax.rem(z, 2) == 0)
    def _():
        rest(0)

    @pl.when(lax.rem(z, 2) == 1)
    def _():
        rest(1)

    local = [pltpu.make_async_copy(p_hbm, p_s, small.at[0]), pltpu.make_async_copy(bits_hbm, bits_s, small.at[1]),
             pltpu.make_async_copy(block(x_hbm, z, None), block(rows_t, z, None), small.at[2])]
    for copy in local:
        copy.start()

    depth, lanes = b_hbm.shape[3], b_hbm.shape[4]
    half = group // 2
    quarter = half // 2

    def arrived(s):
        pull(s).wait()
        push(s).wait_recv()

    def pair(h, s, uh, at):
        return jnp.concatenate([parts[uh, s, 0, h, at, :], parts[uh, s, 1, h, at, :]], axis=1)

    def one_hot(shape, hit):
        return jnp.where(hit(lax.broadcasted_iota(jnp.int32, shape, 0), lax.broadcasted_iota(jnp.int32, shape, 1)), 1.0, 0.0).astype(BF16)

    def prepare_even(i, s):
        perm = one_hot((2 * half, 2 * half), lambda j, r: r == (j % quarter) * 4 + j // quarter)
        for h in range(2):
            for uh in range(2):
                for ub in range(2):
                    got = dot(perm, pair(h, s, uh, pl.ds(ub * 4 * quarter, 4 * quarter))).astype(BF16)
                    for wt in range(2):
                        for g in range(2):
                            k = (wt * 2 + g) * quarter
                            re, im = got[k:k + quarter, :lanes], got[k:k + quarter, lanes:]
                            u = uh * half + ub * quarter
                            for p, q, what in ((0, 0, re), (0, 1, im), (1, 0, -im), (1, 1, re)):
                                even_w[i, pl.ds((p * 2 + h) * group + u, quarter), pl.ds((q * 2 + g) * group + wt * lanes, lanes)] = what

    def prepare_odd(i, s):
        perm = one_hot((depth, depth), lambda r, j: r == (j % half) * 4 + j // half)
        for h in range(2):
            for uh in range(2):
                got = dot(pair(h, s, uh, slice(None)), perm, ((0,), (0,))).astype(BF16)
                for wt in range(2):
                    for g in range(2):
                        k = (wt * 2 + g) * half
                        re, im = got[:lanes, k:k + half], got[lanes:, k:k + half]
                        for p, q, what in ((0, 0, re), (0, 1, im), (1, 0, -im), (1, 1, re)):
                            odd_w[i, pl.ds((q * 2 + g) * group + wt * lanes, lanes), pl.ds((p * 2 + h) * group + uh * half, half)] = what

    def prepare(i, _):
        arrived(2 * i)
        prepare_even(i, 2 * i)
        arrived(2 * i + 1)
        prepare_odd(i, 2 * i + 1)
        return 0

    lax.fori_loop(0, 3, prepare, 0)
    arrived(6)
    prepare_odd(3, 6)

    for copy in local:
        copy.wait()

    def project(s, g, y_re, y_im):
        one = bits_s[0, s] == 1
        p_re = jnp.where(one, p_s[1, 0, g, s], p_s[0, 0, g, s])
        p_im = jnp.where(one, p_s[1, 1, g, s], p_s[0, 1, g, s])
        return p_re * y_re - p_im * y_im, p_re * y_im + p_im * y_re

    def at(q, g):
        return pl.ds((q * 2 + g) * group, group)

    for copy in first:
        copy.wait_recv()

    def two_steps(i, _):
        for g in range(2):
            z_re, z_im = project(2 * i, g, dot(rows_t[...], even_w[i, :, at(0, g)]), dot(rows_t[...], even_w[i, :, at(1, g)]))
            rows[at(0, g), :] = z_re.astype(BF16)
            rows[at(1, g), :] = z_im.astype(BF16)
        for g in range(2):
            z_re, z_im = project(2 * i + 1, g, dot(odd_w[i, at(0, g), :], rows[...]), dot(odd_w[i, at(1, g), :], rows[...]))
            rows_t[:, at(0, g)] = z_re.astype(BF16)
            rows_t[:, at(1, g)] = z_im.astype(BF16)
        return 0

    lax.fori_loop(0, 3, two_steps, 0)
    for g in range(2):
        z_re, z_im = project(6, g, dot(odd_w[3, at(0, g), :], rows_t[...], ((1,), (1,))),
                             dot(odd_w[3, at(1, g), :], rows_t[...], ((1,), (1,))))
        send[:, at(0, g)] = z_re.astype(BF16)
        send[:, at(1, g)] = z_im.astype(BF16)

    second = exchange(send, last, send2, recv2)
    for copy in second:
        copy.start()
    own = pltpu.make_async_copy(block(send, z, None), block(last, z, None), small.at[0])
    own.start()
    arrived(7)
    prepare_even(3, 7)
    for s in range(steps):
        push(s).wait_send()
    for copy in first:
        copy.wait_send()
    own.wait()
    for copy in second:
        copy.wait_recv()
    for g in range(2):
        z_re, z_im = project(7, g, dot(last[...], even_w[3, :, at(0, g)]), dot(last[...], even_w[3, :, at(1, g)]))
        out[0, :, 0, g] = z_re.reshape(n, wide, group)
        out[0, :, 1, g] = z_im.reshape(n, wide, group)
    for copy in second:
        copy.wait_send()


def shards(n, initial, branches, projectors, bits):
    _, columns, _, _, group, wide = initial.shape
    steps, _, _, half, _, _ = branches.shape
    x = initial[0].transpose(0, 4, 1, 2, 3).reshape(columns * wide, 4 * group)
    b = branches.reshape(steps, 2, 2, half, 2, 2, group // 2).transpose(0, 1, 2, 3, 5, 4, 6).reshape(steps, 2, 2, half * 4, group // 2)
    hops = len(hops_of(n))
    return pl.pallas_call(
        functools.partial(kernel, n),
        out_shape=jax.ShapeDtypeStruct((1, columns, 2, 2, wide, group), F32),
        in_specs=[pl.BlockSpec(memory_space=pl.ANY)] * 4,
        out_specs=pl.BlockSpec(memory_space=pltpu.VMEM),
        scratch_shapes=[
            pltpu.VMEM((2, steps, 2, 2, half * 4, group // 2), BF16),
            pltpu.VMEM((4, 4 * group, 4 * group), BF16),
            pltpu.VMEM((4, 4 * group, 4 * group), BF16),
            pltpu.VMEM((group, 4 * group), BF16),
            pltpu.VMEM((4 * group, group), BF16),
            pltpu.VMEM((group, 4 * group), BF16),
            pltpu.VMEM((group, 4 * group), BF16),
            pltpu.SMEM((2, 2, 2, steps), F32),
            pltpu.SMEM((1, steps), jnp.int32),
            pltpu.SemaphoreType.DMA((hops,)),
            pltpu.SemaphoreType.DMA((hops,)),
            pltpu.SemaphoreType.DMA((hops,)),
            pltpu.SemaphoreType.DMA((hops,)),
            pltpu.SemaphoreType.DMA((steps,)),
            pltpu.SemaphoreType.DMA((steps,)),
            pltpu.SemaphoreType.DMA((steps,)),
            pltpu.SemaphoreType.DMA((3,)),
            pltpu.SemaphoreType.REGULAR((len(chain_of(n)), 2)),
        ],
        compiler_params=pltpu.CompilerParams(collective_id=0, has_side_effects=True, vmem_limit_bytes=60 * 2**20),
    )(x, b, projectors.transpose(1, 2, 3, 0), bits)


def solution(mesh):
    in_specs = (
        P("batch", "cuts", None, None, None, "wide"),
        P(None, None, None, "batch", None, None),
        P(),
        P("batch", None),
    )
    out_specs = P("batch", "cuts", None, None, "wide", None)
    return jax.shard_map(functools.partial(shards, mesh.shape["wide"]), mesh=mesh, in_specs=in_specs, out_specs=out_specs, check_vma=False)
```

```python
import functools

import jax
import jax.numpy as jnp
from jax import lax
from jax.experimental import pallas as pl
from jax.experimental.pallas import tpu as pltpu
from jax.sharding import PartitionSpec as P

MESH = pl.DeviceIdType.MESH
BF16, F32 = jnp.bfloat16, jnp.float32


def dot(a, b, dims=((1,), (0,))):
    return lax.dot_general(a, b, (dims, ((), ())), preferred_element_type=F32)


def hops_of(n):
    order = [(n // 2, 0), (-(n // 2), 1)]
    for far in range(n // 2 - 1, 0, -1):
        order += [(far, None), (-far, None)]
    return order


NEAR = 3
EARLY = 8


def chain_of(n):
    reach, rounds = min(NEAR, n // 2), []
    while reach < n // 2:
        rounds.append(min(reach, n // 2 - reach))
        reach += rounds[-1]
    return rounds


def kernel(n, x_hbm, b_hbm, p_hbm, bits_hbm, last, final_w, final_p, parts, even_w, odd_w, rows_t, rows, send, p_s, bits_s,
           send1, recv1, send2, recv2, bsend, brecv, bown, small, chain):
    z = lax.axis_index("wide")
    core = lax.axis_index("batch")
    wide, cols = x_hbm.shape[0] // n, x_hbm.shape[1]
    group = cols // 4
    steps = b_hbm.shape[0]
    hops = hops_of(n)

    barrier = pltpu.get_barrier_semaphore()
    pl.semaphore_signal(barrier, inc=1, device_id={"batch": 1 - core}, device_id_type=MESH)
    for d in range(1, NEAR + 1):
        for to in (d, n - d):
            pl.semaphore_signal(barrier, inc=1, device_id={"wide": lax.rem(z + to, n)}, device_id_type=MESH)
    pl.semaphore_wait(barrier, 2 * NEAR + 1)

    def block(ref, index, piece):
        at = pl.ds(pl.multiple_of(index * wide, wide), wide)
        if piece is None:
            return ref.at[at, :]
        return ref.at[at, pl.ds(piece * (cols // 2), cols // 2)]

    def exchange(src, dst, ssem, rsem):
        copies = []
        for i, (d, piece) in enumerate(hops):
            to = lax.rem(z + d + n, n)
            copies.append(pltpu.make_async_remote_copy(
                src_ref=block(src, to, piece), dst_ref=block(dst, z, piece), send_sem=ssem.at[i], recv_sem=rsem.at[i],
                device_id={"wide": to}, device_id_type=MESH))
        return copies

    def push(s):
        return pltpu.make_async_remote_copy(
            src_ref=b_hbm.at[s], dst_ref=parts.at[core, s], send_sem=bsend.at[s], recv_sem=brecv.at[s],
            device_id={"batch": 1 - core}, device_id_type=MESH)

    def pull(s):
        return pltpu.make_async_copy(b_hbm.at[s], parts.at[core, s], bown.at[s])

    first = exchange(x_hbm, rows_t, send1, recv1)

    def start(nearest, farthest):
        for (d, _), copy in reversed(list(zip(hops, first))):
            if nearest <= abs(d) <= farthest:
                copy.start()

    rounds = chain_of(n)

    def greet(k):
        if k < len(rounds):
            for way, to in enumerate((rounds[k], n - rounds[k])):
                pl.semaphore_signal(chain.at[k, way], inc=1, device_id={"wide": lax.rem(z + to, n)}, device_id_type=MESH)

    reach = NEAR
    greet(0)
    start(1, min(reach, EARLY))
    for s in range(steps):
        push(s).start()
        pull(s).start()
    for k, hop in enumerate(rounds):
        for way in range(2):
            pl.semaphore_wait(chain.at[k, way], 1)
        greet(k + 1)
        start(reach + 1, min(reach + hop, EARLY))
        reach += hop

    def rest(odd):
        for dests in (0, 1):
            for (d, _), copy in zip(hops, first):
                if abs(d) > EARLY and (d + odd + dests) % 2 == 0:
                    copy.start()

    @pl.when(lax.rem(z + core, 2) == 0)
    def _():
        rest(0)

    @pl.when(lax.rem(z + core, 2) == 1)
    def _():
        rest(1)

    local = [pltpu.make_async_copy(p_hbm, p_s, small.at[0]), pltpu.make_async_copy(bits_hbm, bits_s, small.at[1]),
             pltpu.make_async_copy(block(x_hbm, z, None), block(rows_t, z, None), small.at[2])]
    for copy in local:
        copy.start()

    depth, lanes = b_hbm.shape[3], b_hbm.shape[4]
    half = group // 2
    quarter = half // 2

    def arrived(s):
        pull(s).wait()
        push(s).wait_recv()

    def pair(h, s, uh, at):
        return jnp.concatenate([parts[uh, s, 0, h, at, :], parts[uh, s, 1, h, at, :]], axis=1)

    def one_hot(shape, hit):
        return jnp.where(hit(lax.broadcasted_iota(jnp.int32, shape, 0), lax.broadcasted_iota(jnp.int32, shape, 1)), 1.0, 0.0).astype(BF16)

    def prepare_even(into, s):
        perm = one_hot((2 * half, 2 * half), lambda j, r: r == (j % quarter) * 4 + j // quarter)
        for h in range(2):
            for uh in range(2):
                for ub in range(2):
                    got = dot(perm, pair(h, s, uh, pl.ds(ub * 4 * quarter, 4 * quarter))).astype(BF16)
                    for wt in range(2):
                        for g in range(2):
                            k = (wt * 2 + g) * quarter
                            re, im = got[k:k + quarter, :lanes], got[k:k + quarter, lanes:]
                            u = uh * half + ub * quarter
                            for p, q, what in ((0, 0, re), (0, 1, im), (1, 0, -im), (1, 1, re)):
                                into[pl.ds((p * 2 + h) * group + u, quarter), pl.ds((q * 2 + g) * group + wt * lanes, lanes)] = what

    def prepare_odd(i, s):
        perm = one_hot((depth, depth), lambda r, j: r == (j % half) * 4 + j // half)
        for h in range(2):
            for uh in range(2):
                got = dot(pair(h, s, uh, slice(None)), perm, ((0,), (0,))).astype(BF16)
                for wt in range(2):
                    for g in range(2):
                        k = (wt * 2 + g) * half
                        re, im = got[:lanes, k:k + half], got[lanes:, k:k + half]
                        for p, q, what in ((0, 0, re), (0, 1, im), (1, 0, -im), (1, 1, re)):
                            odd_w[i, pl.ds((q * 2 + g) * group + wt * lanes, lanes), pl.ds((p * 2 + h) * group + uh * half, half)] = what

    def prepare(i, _):
        arrived(2 * i)
        prepare_even(even_w.at[i], 2 * i)
        arrived(2 * i + 1)
        prepare_odd(i, 2 * i + 1)
        return 0

    lax.fori_loop(0, 3, prepare, 0)
    arrived(6)
    prepare_odd(3, 6)

    for copy in local:
        copy.wait()

    def chosen(s, part, g):
        return jnp.where(bits_s[0, s] == 1, p_s[1, part, g, s], p_s[0, part, g, s])

    def project(s, g, y_re, y_im):
        p_re, p_im = chosen(s, 0, g), chosen(s, 1, g)
        return p_re * y_re - p_im * y_im, p_re * y_im + p_im * y_re

    def at(q, g):
        return pl.ds((q * 2 + g) * group, group)

    for copy in first:
        copy.wait_recv()

    def two_steps(i, _):
        for g in range(2):
            z_re, z_im = project(2 * i, g, dot(rows_t[...], even_w[i, :, at(0, g)]), dot(rows_t[...], even_w[i, :, at(1, g)]))
            rows[at(0, g), :] = z_re.astype(BF16)
            rows[at(1, g), :] = z_im.astype(BF16)
        for g in range(2):
            z_re, z_im = project(2 * i + 1, g, dot(odd_w[i, at(0, g), :], rows[...]), dot(odd_w[i, at(1, g), :], rows[...]))
            rows_t[:, at(0, g)] = z_re.astype(BF16)
            rows_t[:, at(1, g)] = z_im.astype(BF16)
        return 0

    lax.fori_loop(0, 3, two_steps, 0)
    for g in range(2):
        z_re, z_im = project(6, g, dot(odd_w[3, at(0, g), :], rows_t[...], ((1,), (1,))),
                             dot(odd_w[3, at(1, g), :], rows_t[...], ((1,), (1,))))
        send[:, at(0, g)] = z_re.astype(BF16)
        send[:, at(1, g)] = z_im.astype(BF16)

    second = exchange(send, last, send2, recv2)
    for copy in second:
        copy.start()
    own = pltpu.make_async_copy(block(send, z, None), block(last, z, None), small.at[0])
    own.start()
    arrived(7)
    prepare_even(final_w, 7)
    for part in range(2):
        for g in range(2):
            final_p[:, at(part, g)] = jnp.zeros((8, group), F32) + chosen(7, part, g)
    for s in range(steps):
        push(s).wait_send()
    for copy in first:
        copy.wait_send()
    own.wait()
    for copy in second:
        copy.wait_recv()
    for copy in second:
        copy.wait_send()


def final_kernel(last, weights, p, out, held, sems):
    columns, _, _, wide, group = held.shape

    def at(q, g):
        return pl.ds((q * 2 + g) * group, group)

    copies = []
    for g in range(2):
        y_re, y_im = dot(last[...], weights[:, at(0, g)]), dot(last[...], weights[:, at(1, g)])
        p_re, p_im = p[0:1, at(0, g)], p[0:1, at(1, g)]
        held[:, 0, g] = (p_re * y_re - p_im * y_im).reshape(columns, wide, group)
        held[:, 1, g] = (p_re * y_im + p_im * y_re).reshape(columns, wide, group)
        copies.append(pltpu.make_async_copy(held.at[:, :, g], out.at[0, :, :, g], sems.at[g]))
        copies[-1].start()
    for copy in copies:
        copy.wait()


def shards(n, initial, branches, projectors, bits):
    _, columns, _, _, group, wide = initial.shape
    steps, _, _, half, _, _ = branches.shape
    x = initial[0].transpose(0, 4, 1, 2, 3).reshape(columns * wide, 4 * group)
    b = branches.reshape(steps, 2, 2, half, 2, 2, group // 2).transpose(0, 1, 2, 3, 5, 4, 6).reshape(steps, 2, 2, half * 4, group // 2)
    hops = len(hops_of(n))
    last, weights, p = pl.pallas_call(
        functools.partial(kernel, n),
        out_shape=[
            jax.ShapeDtypeStruct((group, 4 * group), BF16),
            jax.ShapeDtypeStruct((4 * group, 4 * group), BF16),
            jax.ShapeDtypeStruct((8, 4 * group), F32),
        ],
        in_specs=[pl.BlockSpec(memory_space=pltpu.HBM)] * 4,
        out_specs=[pl.BlockSpec(memory_space=pltpu.VMEM)] * 3,
        scratch_shapes=[
            pltpu.VMEM((2, steps, 2, 2, half * 4, group // 2), BF16),
            pltpu.VMEM((3, 4 * group, 4 * group), BF16),
            pltpu.VMEM((4, 4 * group, 4 * group), BF16),
            pltpu.VMEM((group, 4 * group), BF16),
            pltpu.VMEM((4 * group, group), BF16),
            pltpu.VMEM((group, 4 * group), BF16),
            pltpu.SMEM((2, 2, 2, steps), F32),
            pltpu.SMEM((1, steps), jnp.int32),
            pltpu.SemaphoreType.DMA((hops,)),
            pltpu.SemaphoreType.DMA((hops,)),
            pltpu.SemaphoreType.DMA((hops,)),
            pltpu.SemaphoreType.DMA((hops,)),
            pltpu.SemaphoreType.DMA((steps,)),
            pltpu.SemaphoreType.DMA((steps,)),
            pltpu.SemaphoreType.DMA((steps,)),
            pltpu.SemaphoreType.DMA((3,)),
            pltpu.SemaphoreType.REGULAR((len(chain_of(n)), 2)),
        ],
        compiler_params=pltpu.CompilerParams(collective_id=0, has_side_effects=True, vmem_limit_bytes=40 * 2**20),
    )(*(pltpu.with_memory_space_constraint(a, pltpu.HBM) for a in (x, b, projectors.transpose(1, 2, 3, 0), bits)))
    return pl.pallas_call(
        final_kernel,
        out_shape=jax.ShapeDtypeStruct((1, columns, 2, 2, wide, group), F32),
        in_specs=[pl.BlockSpec(memory_space=pltpu.VMEM)] * 3,
        out_specs=pl.BlockSpec(memory_space=pl.ANY),
        scratch_shapes=[pltpu.VMEM((columns, 2, 2, wide, group), F32), pltpu.SemaphoreType.DMA((2,))],
        compiler_params=pltpu.CompilerParams(vmem_limit_bytes=16 * 2**20),
    )(last, weights, p)


def solution(mesh):
    in_specs = (
        P("batch", "cuts", None, None, None, "wide"),
        P(None, None, None, "batch", None, None),
        P(),
        P("batch", None),
    )
    out_specs = P("batch", "cuts", None, None, "wide", None)
    return jax.shard_map(functools.partial(shards, mesh.shape["wide"]), mesh=mesh, in_specs=in_specs, out_specs=out_specs, check_vma=False)
```

```python
import functools

import jax
import jax.numpy as jnp
from jax import lax
from jax.experimental import pallas as pl
from jax.experimental.pallas import tpu as pltpu
from jax.sharding import PartitionSpec as P

MESH = pl.DeviceIdType.MESH
BF16, F32 = jnp.bfloat16, jnp.float32


def dot(a, b, dims=((1,), (0,))):
    return lax.dot_general(a, b, (dims, ((), ())), preferred_element_type=F32)


def hops_of(n):
    order = [(n // 2, 0), (-(n // 2), 1)]
    for far in range(n // 2 - 1, 0, -1):
        order += [(far, None), (-far, None)]
    return order


NEAR = 3
EARLY = 8


def chain_of(n):
    reach, rounds = min(NEAR, n // 2), []
    while reach < n // 2:
        rounds.append(min(reach, n // 2 - reach))
        reach += rounds[-1]
    return rounds


def kernel(n, x_hbm, b_hbm, p_hbm, bits_hbm, last, final_w, final_p, parts, even_w, odd_w, rows_t, rows, send, p_s, bits_s,
           send1, recv1, send2, recv2, bsend, brecv, bown, small, chain):
    z = lax.axis_index("wide")
    core = lax.axis_index("batch")
    wide, cols = x_hbm.shape[0] // n, x_hbm.shape[1]
    group = cols // 4
    steps = b_hbm.shape[0]
    hops = hops_of(n)

    barrier = pltpu.get_barrier_semaphore()
    pl.semaphore_signal(barrier, inc=1, device_id={"batch": 1 - core}, device_id_type=MESH)
    for d in range(1, NEAR + 1):
        for to in (d, n - d):
            pl.semaphore_signal(barrier, inc=1, device_id={"wide": lax.rem(z + to, n)}, device_id_type=MESH)
    pl.semaphore_wait(barrier, 2 * NEAR + 1)

    def block(ref, index, piece):
        at = pl.ds(pl.multiple_of(index * wide, wide), wide)
        if piece is None:
            return ref.at[at, :]
        return ref.at[at, pl.ds(piece * (cols // 2), cols // 2)]

    def exchange(src, dst, ssem, rsem):
        copies = []
        for i, (d, piece) in enumerate(hops):
            to = lax.rem(z + d + n, n)
            copies.append(pltpu.make_async_remote_copy(
                src_ref=block(src, to, piece), dst_ref=block(dst, z, piece), send_sem=ssem.at[i], recv_sem=rsem.at[i],
                device_id={"wide": to}, device_id_type=MESH))
        return copies

    def push(s):
        return pltpu.make_async_remote_copy(
            src_ref=b_hbm.at[s], dst_ref=parts.at[core, s], send_sem=bsend.at[s], recv_sem=brecv.at[s],
            device_id={"batch": 1 - core}, device_id_type=MESH)

    def pull(s):
        return pltpu.make_async_copy(b_hbm.at[s], parts.at[core, s], bown.at[s])

    first = exchange(x_hbm, rows_t, send1, recv1)

    def start(nearest, farthest):
        for (d, _), copy in zip(hops, first):
            if nearest <= abs(d) <= farthest:
                copy.start()

    rounds = chain_of(n)

    def greet(k):
        if k < len(rounds):
            for way, to in enumerate((rounds[k], n - rounds[k])):
                pl.semaphore_signal(chain.at[k, way], inc=1, device_id={"wide": lax.rem(z + to, n)}, device_id_type=MESH)

    reach = NEAR
    greet(0)
    start(1, min(reach, EARLY))
    for s in range(steps):
        push(s).start()
        pull(s).start()
    for k, hop in enumerate(rounds):
        for way in range(2):
            pl.semaphore_wait(chain.at[k, way], 1)
        greet(k + 1)
        start(reach + 1, min(reach + hop, EARLY))
        reach += hop

    def rest(odd):
        for dests in (0, 1):
            for (d, _), copy in zip(hops, first):
                if abs(d) > EARLY and (d + odd + dests) % 2 == 0:
                    copy.start()

    @pl.when(lax.rem(z + core, 2) == 0)
    def _():
        rest(0)

    @pl.when(lax.rem(z + core, 2) == 1)
    def _():
        rest(1)

    local = [pltpu.make_async_copy(p_hbm, p_s, small.at[0]), pltpu.make_async_copy(bits_hbm, bits_s, small.at[1]),
             pltpu.make_async_copy(block(x_hbm, z, None), block(rows_t, z, None), small.at[2])]
    for copy in local:
        copy.start()

    depth, lanes = b_hbm.shape[3], b_hbm.shape[4]
    half = group // 2
    quarter = half // 2

    def arrived(s):
        pull(s).wait()
        push(s).wait_recv()

    def pair(h, s, uh, at):
        return jnp.concatenate([parts[uh, s, 0, h, at, :], parts[uh, s, 1, h, at, :]], axis=1)

    def one_hot(shape, hit):
        return jnp.where(hit(lax.broadcasted_iota(jnp.int32, shape, 0), lax.broadcasted_iota(jnp.int32, shape, 1)), 1.0, 0.0).astype(BF16)

    def prepare_even(into, s):
        perm = one_hot((2 * half, 2 * half), lambda j, r: r == (j % quarter) * 4 + j // quarter)
        for h in range(2):
            for uh in range(2):
                for ub in range(2):
                    got = dot(perm, pair(h, s, uh, pl.ds(ub * 4 * quarter, 4 * quarter))).astype(BF16)
                    for wt in range(2):
                        for g in range(2):
                            k = (wt * 2 + g) * quarter
                            re, im = got[k:k + quarter, :lanes], got[k:k + quarter, lanes:]
                            u = uh * half + ub * quarter
                            for p, q, what in ((0, 0, re), (0, 1, im), (1, 0, -im), (1, 1, re)):
                                into[pl.ds((p * 2 + h) * group + u, quarter), pl.ds((q * 2 + g) * group + wt * lanes, lanes)] = what

    def prepare_odd(i, s):
        perm = one_hot((depth, depth), lambda r, j: r == (j % half) * 4 + j // half)
        for h in range(2):
            for uh in range(2):
                got = dot(pair(h, s, uh, slice(None)), perm, ((0,), (0,))).astype(BF16)
                for wt in range(2):
                    for g in range(2):
                        k = (wt * 2 + g) * half
                        re, im = got[:lanes, k:k + half], got[lanes:, k:k + half]
                        for p, q, what in ((0, 0, re), (0, 1, im), (1, 0, -im), (1, 1, re)):
                            odd_w[i, pl.ds((q * 2 + g) * group + wt * lanes, lanes), pl.ds((p * 2 + h) * group + uh * half, half)] = what

    def prepare(i, _):
        arrived(2 * i)
        prepare_even(even_w.at[i], 2 * i)
        arrived(2 * i + 1)
        prepare_odd(i, 2 * i + 1)
        return 0

    lax.fori_loop(0, 3, prepare, 0)
    arrived(6)
    prepare_odd(3, 6)

    for copy in local:
        copy.wait()

    def chosen(s, part, g):
        return jnp.where(bits_s[0, s] == 1, p_s[1, part, g, s], p_s[0, part, g, s])

    def project(s, g, y_re, y_im):
        p_re, p_im = chosen(s, 0, g), chosen(s, 1, g)
        return p_re * y_re - p_im * y_im, p_re * y_im + p_im * y_re

    def at(q, g):
        return pl.ds((q * 2 + g) * group, group)

    for copy in first:
        copy.wait_recv()

    def two_steps(i, _):
        for g in range(2):
            z_re, z_im = project(2 * i, g, dot(rows_t[...], even_w[i, :, at(0, g)]), dot(rows_t[...], even_w[i, :, at(1, g)]))
            rows[at(0, g), :] = z_re.astype(BF16)
            rows[at(1, g), :] = z_im.astype(BF16)
        for g in range(2):
            z_re, z_im = project(2 * i + 1, g, dot(odd_w[i, at(0, g), :], rows[...]), dot(odd_w[i, at(1, g), :], rows[...]))
            rows_t[:, at(0, g)] = z_re.astype(BF16)
            rows_t[:, at(1, g)] = z_im.astype(BF16)
        return 0

    lax.fori_loop(0, 3, two_steps, 0)
    for g in range(2):
        z_re, z_im = project(6, g, dot(odd_w[3, at(0, g), :], rows_t[...], ((1,), (1,))),
                             dot(odd_w[3, at(1, g), :], rows_t[...], ((1,), (1,))))
        send[:, at(0, g)] = z_re.astype(BF16)
        send[:, at(1, g)] = z_im.astype(BF16)

    second = exchange(send, last, send2, recv2)
    for copy in second:
        copy.start()
    own = pltpu.make_async_copy(block(send, z, None), block(last, z, None), small.at[0])
    own.start()
    arrived(7)
    prepare_even(final_w, 7)
    for part in range(2):
        for g in range(2):
            final_p[:, at(part, g)] = jnp.zeros((8, group), F32) + chosen(7, part, g)
    for s in range(steps):
        push(s).wait_send()
    for copy in first:
        copy.wait_send()
    own.wait()
    for copy in second:
        copy.wait_recv()
    for copy in second:
        copy.wait_send()


def final_kernel(last, weights, p, out, held, sems):
    columns, _, _, wide, group = held.shape

    def at(q, g):
        return pl.ds((q * 2 + g) * group, group)

    copies = []
    for g in range(2):
        y_re, y_im = dot(last[...], weights[:, at(0, g)]), dot(last[...], weights[:, at(1, g)])
        p_re, p_im = p[0:1, at(0, g)], p[0:1, at(1, g)]
        held[:, 0, g] = (p_re * y_re - p_im * y_im).reshape(columns, wide, group)
        held[:, 1, g] = (p_re * y_im + p_im * y_re).reshape(columns, wide, group)
        copies.append(pltpu.make_async_copy(held.at[:, :, g], out.at[0, :, :, g], sems.at[g]))
        copies[-1].start()
    for copy in copies:
        copy.wait()


def shards(n, initial, branches, projectors, bits):
    _, columns, _, _, group, wide = initial.shape
    steps, _, _, half, _, _ = branches.shape
    x = initial[0].transpose(0, 4, 1, 2, 3).reshape(columns * wide, 4 * group)
    b = branches.reshape(steps, 2, 2, half, 2, 2, group // 2).transpose(0, 1, 2, 3, 5, 4, 6).reshape(steps, 2, 2, half * 4, group // 2)
    hops = len(hops_of(n))
    last, weights, p = pl.pallas_call(
        functools.partial(kernel, n),
        out_shape=[
            jax.ShapeDtypeStruct((group, 4 * group), BF16),
            jax.ShapeDtypeStruct((4 * group, 4 * group), BF16),
            jax.ShapeDtypeStruct((8, 4 * group), F32),
        ],
        in_specs=[pl.BlockSpec(memory_space=pltpu.HBM)] * 4,
        out_specs=[pl.BlockSpec(memory_space=pltpu.VMEM)] * 3,
        scratch_shapes=[
            pltpu.VMEM((2, steps, 2, 2, half * 4, group // 2), BF16),
            pltpu.VMEM((3, 4 * group, 4 * group), BF16),
            pltpu.VMEM((4, 4 * group, 4 * group), BF16),
            pltpu.VMEM((group, 4 * group), BF16),
            pltpu.VMEM((4 * group, group), BF16),
            pltpu.VMEM((group, 4 * group), BF16),
            pltpu.SMEM((2, 2, 2, steps), F32),
            pltpu.SMEM((1, steps), jnp.int32),
            pltpu.SemaphoreType.DMA((hops,)),
            pltpu.SemaphoreType.DMA((hops,)),
            pltpu.SemaphoreType.DMA((hops,)),
            pltpu.SemaphoreType.DMA((hops,)),
            pltpu.SemaphoreType.DMA((steps,)),
            pltpu.SemaphoreType.DMA((steps,)),
            pltpu.SemaphoreType.DMA((steps,)),
            pltpu.SemaphoreType.DMA((3,)),
            pltpu.SemaphoreType.REGULAR((len(chain_of(n)), 2)),
        ],
        compiler_params=pltpu.CompilerParams(collective_id=0, has_side_effects=True, vmem_limit_bytes=40 * 2**20),
    )(*(pltpu.with_memory_space_constraint(a, pltpu.HBM) for a in (x, b, projectors.transpose(1, 2, 3, 0), bits)))
    return pl.pallas_call(
        final_kernel,
        out_shape=jax.ShapeDtypeStruct((1, columns, 2, 2, wide, group), F32),
        in_specs=[pl.BlockSpec(memory_space=pltpu.VMEM)] * 3,
        out_specs=pl.BlockSpec(memory_space=pl.ANY),
        scratch_shapes=[pltpu.VMEM((columns, 2, 2, wide, group), F32), pltpu.SemaphoreType.DMA((2,))],
        compiler_params=pltpu.CompilerParams(vmem_limit_bytes=16 * 2**20),
    )(last, weights, p)


def solution(mesh):
    in_specs = (
        P("batch", "cuts", None, None, None, "wide"),
        P(None, None, None, "batch", None, None),
        P(),
        P("batch", None),
    )
    out_specs = P("batch", "cuts", None, None, "wide", None)
    return jax.shard_map(functools.partial(shards, mesh.shape["wide"]), mesh=mesh, in_specs=in_specs, out_specs=out_specs, check_vma=False)
```

```python
import functools

import jax
import jax.numpy as jnp
from jax import lax
from jax.experimental import pallas as pl
from jax.experimental.pallas import tpu as pltpu
from jax.sharding import PartitionSpec as P

MESH = pl.DeviceIdType.MESH
BF16, F32 = jnp.bfloat16, jnp.float32


def dot(a, b, dims=((1,), (0,))):
    return lax.dot_general(a, b, (dims, ((), ())), preferred_element_type=F32)


def hops_of(n):
    order = [(n // 2, 0), (-(n // 2), 1)]
    for far in range(n // 2 - 1, 0, -1):
        order += [(far, None), (-far, None)]
    return order


NEAR = 3
EARLY = 8


def chain_of(n):
    reach, rounds = min(NEAR, n // 2), []
    while reach < n // 2:
        rounds.append(min(reach, n // 2 - reach))
        reach += rounds[-1]
    return rounds


def kernel(n, x_hbm, b_hbm, p_hbm, bits_hbm, last, final_w, final_p, parts, even_w, odd_w, rows_t, rows, send, p_s, bits_s,
           send1, recv1, send2, recv2, bsend, brecv, bown, small, chain):
    z = lax.axis_index("wide")
    core = lax.axis_index("batch")
    wide, cols = x_hbm.shape[0] // n, x_hbm.shape[1]
    group = cols // 4
    steps = b_hbm.shape[0]
    hops = hops_of(n)

    barrier = pltpu.get_barrier_semaphore()
    pl.semaphore_signal(barrier, inc=1, device_id={"batch": 1 - core}, device_id_type=MESH)
    for d in range(1, NEAR + 1):
        for to in (d, n - d):
            pl.semaphore_signal(barrier, inc=1, device_id={"wide": lax.rem(z + to, n)}, device_id_type=MESH)
    pl.semaphore_wait(barrier, 2 * NEAR + 1)

    def block(ref, index, piece):
        at = pl.ds(pl.multiple_of(index * wide, wide), wide)
        if piece is None:
            return ref.at[at, :]
        return ref.at[at, pl.ds(piece * (cols // 2), cols // 2)]

    def exchange(src, dst, ssem, rsem):
        copies = []
        for i, (d, piece) in enumerate(hops):
            to = lax.rem(z + d + n, n)
            copies.append(pltpu.make_async_remote_copy(
                src_ref=block(src, to, piece), dst_ref=block(dst, z, piece), send_sem=ssem.at[i], recv_sem=rsem.at[i],
                device_id={"wide": to}, device_id_type=MESH))
        return copies

    def push(s):
        return pltpu.make_async_remote_copy(
            src_ref=b_hbm.at[s], dst_ref=parts.at[core, s], send_sem=bsend.at[s], recv_sem=brecv.at[s],
            device_id={"batch": 1 - core}, device_id_type=MESH)

    def pull(s):
        return pltpu.make_async_copy(b_hbm.at[s], parts.at[core, s], bown.at[s])

    first = exchange(x_hbm, rows_t, send1, recv1)

    def start(nearest, farthest):
        for (d, _), copy in zip(hops, first):
            if nearest <= abs(d) <= farthest:
                copy.start()

    rounds = chain_of(n)

    def greet(k):
        if k < len(rounds):
            for way, to in enumerate((rounds[k], n - rounds[k])):
                pl.semaphore_signal(chain.at[k, way], inc=1, device_id={"wide": lax.rem(z + to, n)}, device_id_type=MESH)

    reach = NEAR
    greet(0)
    start(1, min(reach, EARLY))
    for s in range(steps):
        push(s).start()
        pull(s).start()
    for k, hop in enumerate(rounds):
        for way in range(2):
            pl.semaphore_wait(chain.at[k, way], 1)
        greet(k + 1)
        start(reach + 1, min(reach + hop, EARLY))
        reach += hop

    def rest(odd):
        for dests in (0, 1):
            for (d, _), copy in zip(hops, first):
                if abs(d) > EARLY and (d + odd + dests) % 2 == 0:
                    copy.start()

    @pl.when(lax.rem(z + core, 2) == 0)
    def _():
        rest(0)

    @pl.when(lax.rem(z + core, 2) == 1)
    def _():
        rest(1)

    local = [pltpu.make_async_copy(p_hbm, p_s, small.at[0]), pltpu.make_async_copy(bits_hbm, bits_s, small.at[1]),
             pltpu.make_async_copy(block(x_hbm, z, None), block(rows_t, z, None), small.at[2])]
    for copy in local:
        copy.start()

    depth, lanes = b_hbm.shape[3], b_hbm.shape[4]
    half = group // 2
    quarter = half // 2

    def arrived(s):
        pull(s).wait()
        push(s).wait_recv()

    def pair(h, s, uh, at):
        return jnp.concatenate([parts[uh, s, 0, h, at, :], parts[uh, s, 1, h, at, :]], axis=1)

    def one_hot(shape, hit):
        return jnp.where(hit(lax.broadcasted_iota(jnp.int32, shape, 0), lax.broadcasted_iota(jnp.int32, shape, 1)), 1.0, 0.0).astype(BF16)

    def prepare_even(into, s):
        perm = one_hot((2 * half, 2 * half), lambda j, r: r == (j % quarter) * 4 + j // quarter)
        for h in range(2):
            for uh in range(2):
                for ub in range(2):
                    got = dot(perm, pair(h, s, uh, pl.ds(ub * 4 * quarter, 4 * quarter))).astype(BF16)
                    for wt in range(2):
                        for g in range(2):
                            k = (wt * 2 + g) * quarter
                            re, im = got[k:k + quarter, :lanes], got[k:k + quarter, lanes:]
                            u = uh * half + ub * quarter
                            for p, q, what in ((0, 0, re), (0, 1, im), (1, 0, -im), (1, 1, re)):
                                into[pl.ds((p * 2 + h) * group + u, quarter), pl.ds((q * 2 + g) * group + wt * lanes, lanes)] = what

    def prepare_odd(i, s):
        perm = one_hot((depth, depth), lambda r, j: r == (j % half) * 4 + j // half)
        for h in range(2):
            for uh in range(2):
                got = dot(pair(h, s, uh, slice(None)), perm, ((0,), (0,))).astype(BF16)
                for wt in range(2):
                    for g in range(2):
                        k = (wt * 2 + g) * half
                        re, im = got[:lanes, k:k + half], got[lanes:, k:k + half]
                        for p, q, what in ((0, 0, re), (0, 1, im), (1, 0, -im), (1, 1, re)):
                            odd_w[i, pl.ds((q * 2 + g) * group + wt * lanes, lanes), pl.ds((p * 2 + h) * group + uh * half, half)] = what

    def prepare(i, _):
        arrived(2 * i)
        prepare_even(even_w.at[i], 2 * i)
        arrived(2 * i + 1)
        prepare_odd(i, 2 * i + 1)
        return 0

    lax.fori_loop(0, 3, prepare, 0)
    arrived(6)
    prepare_odd(3, 6)

    for copy in local:
        copy.wait()

    def chosen(s, part, g):
        return jnp.where(bits_s[0, s] == 1, p_s[1, part, g, s], p_s[0, part, g, s])

    def project(s, g, y_re, y_im):
        p_re, p_im = chosen(s, 0, g), chosen(s, 1, g)
        return p_re * y_re - p_im * y_im, p_re * y_im + p_im * y_re

    def at(q, g):
        return pl.ds((q * 2 + g) * group, group)

    for copy in first:
        copy.wait_recv()

    def two_steps(i, _):
        for g in range(2):
            z_re, z_im = project(2 * i, g, dot(rows_t[...], even_w[i, :, at(0, g)]), dot(rows_t[...], even_w[i, :, at(1, g)]))
            rows[at(0, g), :] = z_re.astype(BF16)
            rows[at(1, g), :] = z_im.astype(BF16)
        for g in range(2):
            z_re, z_im = project(2 * i + 1, g, dot(odd_w[i, at(0, g), :], rows[...]), dot(odd_w[i, at(1, g), :], rows[...]))
            rows_t[:, at(0, g)] = z_re.astype(BF16)
            rows_t[:, at(1, g)] = z_im.astype(BF16)
        return 0

    lax.fori_loop(0, 3, two_steps, 0)
    for g in range(2):
        z_re, z_im = project(6, g, dot(odd_w[3, at(0, g), :], rows_t[...], ((1,), (1,))),
                             dot(odd_w[3, at(1, g), :], rows_t[...], ((1,), (1,))))
        send[:, at(0, g)] = z_re.astype(BF16)
        send[:, at(1, g)] = z_im.astype(BF16)

    second = exchange(send, last, send2, recv2)
    for copy in second:
        copy.start()
    own = pltpu.make_async_copy(block(send, z, None), block(last, z, None), small.at[0])
    own.start()
    arrived(7)
    prepare_even(final_w, 7)
    for part in range(2):
        for g in range(2):
            final_p[:, at(part, g)] = jnp.zeros((8, group), F32) + chosen(7, part, g)
    for s in range(steps):
        push(s).wait_send()
    for copy in first:
        copy.wait_send()
    own.wait()
    for copy in second:
        copy.wait_send()
        copy.wait_recv()


def final_kernel(last, weights, p, out, held, sems):
    columns, _, _, wide, group = held.shape

    def at(q, g):
        return pl.ds((q * 2 + g) * group, group)

    copies = []
    part = columns // 2
    for top in (0, part):
        for g in range(2):
            some = last[pl.ds(top * wide, part * wide), :]
            y_re, y_im = dot(some, weights[:, at(0, g)]), dot(some, weights[:, at(1, g)])
            p_re, p_im = p[0:1, at(0, g)], p[0:1, at(1, g)]
            held[pl.ds(top, part), 0, g] = (p_re * y_re - p_im * y_im).reshape(part, wide, group)
            held[pl.ds(top, part), 1, g] = (p_re * y_im + p_im * y_re).reshape(part, wide, group)
            copies.append(pltpu.make_async_copy(held.at[pl.ds(top, part), :, g], out.at[0, pl.ds(top, part), :, g], sems.at[len(copies)]))
            copies[-1].start()
    for copy in copies:
        copy.wait()


def shards(n, initial, branches, projectors, bits):
    _, columns, _, _, group, wide = initial.shape
    steps, _, _, half, _, _ = branches.shape
    x = initial[0].transpose(0, 4, 1, 2, 3).reshape(columns * wide, 4 * group)
    b = branches.reshape(steps, 2, 2, half, 2, 2, group // 2).transpose(0, 1, 2, 3, 5, 4, 6).reshape(steps, 2, 2, half * 4, group // 2)
    hops = len(hops_of(n))
    last, weights, p = pl.pallas_call(
        functools.partial(kernel, n),
        out_shape=[
            jax.ShapeDtypeStruct((group, 4 * group), BF16),
            jax.ShapeDtypeStruct((4 * group, 4 * group), BF16),
            jax.ShapeDtypeStruct((8, 4 * group), F32),
        ],
        in_specs=[pl.BlockSpec(memory_space=pltpu.HBM)] * 4,
        out_specs=[pl.BlockSpec(memory_space=pltpu.VMEM)] * 3,
        scratch_shapes=[
            pltpu.VMEM((2, steps, 2, 2, half * 4, group // 2), BF16),
            pltpu.VMEM((3, 4 * group, 4 * group), BF16),
            pltpu.VMEM((4, 4 * group, 4 * group), BF16),
            pltpu.VMEM((group, 4 * group), BF16),
            pltpu.VMEM((4 * group, group), BF16),
            pltpu.VMEM((group, 4 * group), BF16),
            pltpu.SMEM((2, 2, 2, steps), F32),
            pltpu.SMEM((1, steps), jnp.int32),
            pltpu.SemaphoreType.DMA((hops,)),
            pltpu.SemaphoreType.DMA((hops,)),
            pltpu.SemaphoreType.DMA((hops,)),
            pltpu.SemaphoreType.DMA((hops,)),
            pltpu.SemaphoreType.DMA((steps,)),
            pltpu.SemaphoreType.DMA((steps,)),
            pltpu.SemaphoreType.DMA((steps,)),
            pltpu.SemaphoreType.DMA((3,)),
            pltpu.SemaphoreType.REGULAR((len(chain_of(n)), 2)),
        ],
        compiler_params=pltpu.CompilerParams(collective_id=0, has_side_effects=True, vmem_limit_bytes=40 * 2**20),
    )(*(pltpu.with_memory_space_constraint(a, pltpu.HBM) for a in (x, b, projectors.transpose(1, 2, 3, 0), bits)))
    return pl.pallas_call(
        final_kernel,
        out_shape=jax.ShapeDtypeStruct((1, columns, 2, 2, wide, group), F32),
        in_specs=[pl.BlockSpec(memory_space=pltpu.VMEM)] * 3,
        out_specs=pl.BlockSpec(memory_space=pl.ANY),
        scratch_shapes=[pltpu.VMEM((columns, 2, 2, wide, group), F32), pltpu.SemaphoreType.DMA((4,))],
        compiler_params=pltpu.CompilerParams(vmem_limit_bytes=16 * 2**20),
    )(last, weights, p)


def solution(mesh):
    in_specs = (
        P("batch", "cuts", None, None, None, "wide"),
        P(None, None, None, "batch", None, None),
        P(),
        P("batch", None),
    )
    out_specs = P("batch", "cuts", None, None, "wide", None)
    return jax.shard_map(functools.partial(shards, mesh.shape["wide"]), mesh=mesh, in_specs=in_specs, out_specs=out_specs, check_vma=False)
```

```python
import functools

import jax
import jax.numpy as jnp
from jax import lax
from jax.experimental import pallas as pl
from jax.experimental.pallas import tpu as pltpu
from jax.sharding import PartitionSpec as P

MESH = pl.DeviceIdType.MESH
BF16, F32 = jnp.bfloat16, jnp.float32


def dot(a, b, dims=((1,), (0,))):
    return lax.dot_general(a, b, (dims, ((), ())), preferred_element_type=F32)


def hops_of(n):
    order = [(n // 2, 0), (-(n // 2), 1)]
    for far in range(n // 2 - 1, 0, -1):
        order += [(far, None), (-far, None)]
    return order


NEAR = 3
EARLY = 8


def chain_of(n):
    reach, rounds = min(NEAR, n // 2), []
    while reach < n // 2:
        rounds.append(min(reach, n // 2 - reach))
        reach += rounds[-1]
    return rounds


def kernel(n, x_hbm, b_hbm, p_hbm, bits_hbm, last, final_w, final_p, parts, even_w, odd_w, rows_t, rows, send, p_s, bits_s,
           send1, recv1, send2, recv2, bsend, brecv, bown, small, chain):
    z = lax.axis_index("wide")
    core = lax.axis_index("batch")
    wide, cols = x_hbm.shape[0] // n, x_hbm.shape[1]
    group = cols // 4
    steps = b_hbm.shape[0]
    hops = hops_of(n)

    barrier = pltpu.get_barrier_semaphore()
    pl.semaphore_signal(barrier, inc=1, device_id={"batch": 1 - core}, device_id_type=MESH)
    for d in range(1, NEAR + 1):
        for to in (d, n - d):
            pl.semaphore_signal(barrier, inc=1, device_id={"wide": lax.rem(z + to, n)}, device_id_type=MESH)
    pl.semaphore_wait(barrier, 2 * NEAR + 1)

    def block(ref, index, piece):
        at = pl.ds(pl.multiple_of(index * wide, wide), wide)
        if piece is None:
            return ref.at[at, :]
        return ref.at[at, pl.ds(piece * (cols // 2), cols // 2)]

    def exchange(src, dst, ssem, rsem):
        copies = []
        for i, (d, piece) in enumerate(hops):
            to = lax.rem(z + d + n, n)
            copies.append(pltpu.make_async_remote_copy(
                src_ref=block(src, to, piece), dst_ref=block(dst, z, piece), send_sem=ssem.at[i], recv_sem=rsem.at[i],
                device_id={"wide": to}, device_id_type=MESH))
        return copies

    def push(s):
        return pltpu.make_async_remote_copy(
            src_ref=b_hbm.at[s], dst_ref=parts.at[core, s], send_sem=bsend.at[s], recv_sem=brecv.at[s],
            device_id={"batch": 1 - core}, device_id_type=MESH)

    def pull(s):
        return pltpu.make_async_copy(b_hbm.at[s], parts.at[core, s], bown.at[s])

    first = exchange(x_hbm, rows_t, send1, recv1)

    def start(nearest, farthest):
        for (d, _), copy in zip(hops, first):
            if nearest <= abs(d) <= farthest:
                copy.start()

    rounds = chain_of(n)

    def greet(k):
        if k < len(rounds):
            for way, to in enumerate((rounds[k], n - rounds[k])):
                pl.semaphore_signal(chain.at[k, way], inc=1, device_id={"wide": lax.rem(z + to, n)}, device_id_type=MESH)

    reach = NEAR
    greet(0)
    start(1, min(reach, EARLY))
    for k, hop in enumerate(rounds):
        for way in range(2):
            pl.semaphore_wait(chain.at[k, way], 1)
        greet(k + 1)
        start(reach + 1, min(reach + hop, EARLY))
        reach += hop

    for s in range(steps):
        push(s).start()
        pull(s).start()

    def rest(odd):
        for dests in (0, 1):
            for (d, _), copy in zip(hops, first):
                if abs(d) > EARLY and (d + odd + dests) % 2 == 0:
                    copy.start()

    @pl.when(lax.rem(z + core, 2) == 0)
    def _():
        rest(0)

    @pl.when(lax.rem(z + core, 2) == 1)
    def _():
        rest(1)

    local = [pltpu.make_async_copy(p_hbm, p_s, small.at[0]), pltpu.make_async_copy(bits_hbm, bits_s, small.at[1]),
             pltpu.make_async_copy(block(x_hbm, z, None), block(rows_t, z, None), small.at[2])]
    for copy in local:
        copy.start()

    depth, lanes = b_hbm.shape[3], b_hbm.shape[4]
    half = group // 2
    quarter = half // 2

    def arrived(s):
        pull(s).wait()
        push(s).wait_recv()

    def pair(h, s, uh, at):
        return jnp.concatenate([parts[uh, s, 0, h, at, :], parts[uh, s, 1, h, at, :]], axis=1)

    def one_hot(shape, hit):
        return jnp.where(hit(lax.broadcasted_iota(jnp.int32, shape, 0), lax.broadcasted_iota(jnp.int32, shape, 1)), 1.0, 0.0).astype(BF16)

    def prepare_even(into, s):
        perm = one_hot((2 * half, 2 * half), lambda j, r: r == (j % quarter) * 4 + j // quarter)
        for h in range(2):
            for uh in range(2):
                for ub in range(2):
                    got = dot(perm, pair(h, s, uh, pl.ds(ub * 4 * quarter, 4 * quarter))).astype(BF16)
                    for wt in range(2):
                        for g in range(2):
                            k = (wt * 2 + g) * quarter
                            re, im = got[k:k + quarter, :lanes], got[k:k + quarter, lanes:]
                            u = uh * half + ub * quarter
                            for p, q, what in ((0, 0, re), (0, 1, im), (1, 0, -im), (1, 1, re)):
                                into[pl.ds((p * 2 + h) * group + u, quarter), pl.ds((q * 2 + g) * group + wt * lanes, lanes)] = what

    def prepare_odd(i, s):
        perm = one_hot((depth, depth), lambda r, j: r == (j % half) * 4 + j // half)
        for h in range(2):
            for uh in range(2):
                got = dot(pair(h, s, uh, slice(None)), perm, ((0,), (0,))).astype(BF16)
                for wt in range(2):
                    for g in range(2):
                        k = (wt * 2 + g) * half
                        re, im = got[:lanes, k:k + half], got[lanes:, k:k + half]
                        for p, q, what in ((0, 0, re), (0, 1, im), (1, 0, -im), (1, 1, re)):
                            odd_w[i, pl.ds((q * 2 + g) * group + wt * lanes, lanes), pl.ds((p * 2 + h) * group + uh * half, half)] = what

    def prepare(i, _):
        arrived(2 * i)
        prepare_even(even_w.at[i], 2 * i)
        arrived(2 * i + 1)
        prepare_odd(i, 2 * i + 1)
        return 0

    lax.fori_loop(0, 3, prepare, 0)
    arrived(6)
    prepare_odd(3, 6)

    for copy in local:
        copy.wait()

    def chosen(s, part, g):
        return jnp.where(bits_s[0, s] == 1, p_s[1, part, g, s], p_s[0, part, g, s])

    def project(s, g, y_re, y_im):
        p_re, p_im = chosen(s, 0, g), chosen(s, 1, g)
        return p_re * y_re - p_im * y_im, p_re * y_im + p_im * y_re

    def at(q, g):
        return pl.ds((q * 2 + g) * group, group)

    for copy in first:
        copy.wait_recv()

    def two_steps(i, _):
        for g in range(2):
            z_re, z_im = project(2 * i, g, dot(rows_t[...], even_w[i, :, at(0, g)]), dot(rows_t[...], even_w[i, :, at(1, g)]))
            rows[at(0, g), :] = z_re.astype(BF16)
            rows[at(1, g), :] = z_im.astype(BF16)
        for g in range(2):
            z_re, z_im = project(2 * i + 1, g, dot(odd_w[i, at(0, g), :], rows[...]), dot(odd_w[i, at(1, g), :], rows[...]))
            rows_t[:, at(0, g)] = z_re.astype(BF16)
            rows_t[:, at(1, g)] = z_im.astype(BF16)
        return 0

    lax.fori_loop(0, 3, two_steps, 0)
    for g in range(2):
        z_re, z_im = project(6, g, dot(odd_w[3, at(0, g), :], rows_t[...], ((1,), (1,))),
                             dot(odd_w[3, at(1, g), :], rows_t[...], ((1,), (1,))))
        send[:, at(0, g)] = z_re.astype(BF16)
        send[:, at(1, g)] = z_im.astype(BF16)

    second = exchange(send, last, send2, recv2)
    for copy in second:
        copy.start()
    own = pltpu.make_async_copy(block(send, z, None), block(last, z, None), small.at[0])
    own.start()
    arrived(7)
    prepare_even(final_w, 7)
    for part in range(2):
        for g in range(2):
            final_p[:, at(part, g)] = jnp.zeros((8, group), F32) + chosen(7, part, g)
    for s in range(steps):
        push(s).wait_send()
    for copy in first:
        copy.wait_send()
    own.wait()
    for copy in second:
        copy.wait_recv()
    for copy in second:
        copy.wait_send()


def final_kernel(last, weights, p, out, held, sems):
    columns, _, _, wide, group = held.shape

    def at(q, g):
        return pl.ds((q * 2 + g) * group, group)

    copies = []
    for g in range(2):
        y_re, y_im = dot(last[...], weights[:, at(0, g)]), dot(last[...], weights[:, at(1, g)])
        p_re, p_im = p[0:1, at(0, g)], p[0:1, at(1, g)]
        held[:, 0, g] = (p_re * y_re - p_im * y_im).reshape(columns, wide, group)
        held[:, 1, g] = (p_re * y_im + p_im * y_re).reshape(columns, wide, group)
        copies.append(pltpu.make_async_copy(held.at[:, :, g], out.at[0, :, :, g], sems.at[g]))
        copies[-1].start()
    for copy in copies:
        copy.wait()


def shards(n, initial, branches, projectors, bits):
    _, columns, _, _, group, wide = initial.shape
    steps, _, _, half, _, _ = branches.shape
    x = initial[0].transpose(0, 4, 1, 2, 3).reshape(columns * wide, 4 * group)
    b = branches.reshape(steps, 2, 2, half, 2, 2, group // 2).transpose(0, 1, 2, 3, 5, 4, 6).reshape(steps, 2, 2, half * 4, group // 2)
    hops = len(hops_of(n))
    last, weights, p = pl.pallas_call(
        functools.partial(kernel, n),
        out_shape=[
            jax.ShapeDtypeStruct((group, 4 * group), BF16),
            jax.ShapeDtypeStruct((4 * group, 4 * group), BF16),
            jax.ShapeDtypeStruct((8, 4 * group), F32),
        ],
        in_specs=[pl.BlockSpec(memory_space=pltpu.HBM)] * 4,
        out_specs=[pl.BlockSpec(memory_space=pltpu.VMEM)] * 3,
        scratch_shapes=[
            pltpu.VMEM((2, steps, 2, 2, half * 4, group // 2), BF16),
            pltpu.VMEM((3, 4 * group, 4 * group), BF16),
            pltpu.VMEM((4, 4 * group, 4 * group), BF16),
            pltpu.VMEM((group, 4 * group), BF16),
            pltpu.VMEM((4 * group, group), BF16),
            pltpu.VMEM((group, 4 * group), BF16),
            pltpu.SMEM((2, 2, 2, steps), F32),
            pltpu.SMEM((1, steps), jnp.int32),
            pltpu.SemaphoreType.DMA((hops,)),
            pltpu.SemaphoreType.DMA((hops,)),
            pltpu.SemaphoreType.DMA((hops,)),
            pltpu.SemaphoreType.DMA((hops,)),
            pltpu.SemaphoreType.DMA((steps,)),
            pltpu.SemaphoreType.DMA((steps,)),
            pltpu.SemaphoreType.DMA((steps,)),
            pltpu.SemaphoreType.DMA((3,)),
            pltpu.SemaphoreType.REGULAR((len(chain_of(n)), 2)),
        ],
        compiler_params=pltpu.CompilerParams(collective_id=0, has_side_effects=True, vmem_limit_bytes=40 * 2**20),
    )(*(pltpu.with_memory_space_constraint(a, pltpu.HBM) for a in (x, b, projectors.transpose(1, 2, 3, 0), bits)))
    return pl.pallas_call(
        final_kernel,
        out_shape=jax.ShapeDtypeStruct((1, columns, 2, 2, wide, group), F32),
        in_specs=[pl.BlockSpec(memory_space=pltpu.VMEM)] * 3,
        out_specs=pl.BlockSpec(memory_space=pl.ANY),
        scratch_shapes=[pltpu.VMEM((columns, 2, 2, wide, group), F32), pltpu.SemaphoreType.DMA((2,))],
        compiler_params=pltpu.CompilerParams(vmem_limit_bytes=16 * 2**20),
    )(last, weights, p)


def solution(mesh):
    in_specs = (
        P("batch", "cuts", None, None, None, "wide"),
        P(None, None, None, "batch", None, None),
        P(),
        P("batch", None),
    )
    out_specs = P("batch", "cuts", None, None, "wide", None)
    return jax.shard_map(functools.partial(shards, mesh.shape["wide"]), mesh=mesh, in_specs=in_specs, out_specs=out_specs, check_vma=False)
```
